32 devices in a mesh: client: 8 (over z, x), head: 4 (over y, core).
Axes of the slice: x: 2, y: 2, z: 4, core: 2. Of those that a mesh axis runs over, the one named last changes fastest.
Arguments:
- pre: bfloat16 [10240, 4096], P('client'), may hold values from -40 to 40
- delta: float32 [10240, 4096], P('client', 'head'), may hold values from -300 to 300
- head_weight: bfloat16 [4096, 4096], P(None, 'head'), may hold values from -0.09375 to 0.09375
- client_ids: int32 [128], P('client'), may hold values from 0 to 127, as said below
Outputs:
- head_grad: float32 [4096, 4096], P('client', 'head')
- bias_grad: float32 [4096], P('head')
- embed_grad: float32 [128, 4096], P('client', 'head')
- span_grad: float32 [80, 4096], P(None, 'head')
The draws below stay inside these ranges and needn't reach their ends.
Inputs may be any that keep to these rules, and one draw needn't show every extreme that they name: `client_ids`: each of the 128 clients appears exactly once.
All inputs are finite; a program needn't handle non-finite values.
Results may differ from the reference program's by a relative error of at most 0.024.
Values may be sent and summed in bfloat16 or wider, within the bound.
A program may use at most 128 MiB of HBM per device.

```python
import jax
import jax.numpy as jnp
from jax import lax

HID = 4096
EMIT = 4096
SPANS = 80
CLIENTS = 128
ROWS = 10240
N_HEAD = 4


def shuffled_clients(key):
    return jax.random.permutation(jax.random.fold_in(key, 31), CLIENTS).astype(jnp.int32)


def draw_client_ids(key, part):
    return shuffled_clients(key)


def draw_pre(key, part):
    key_base = jax.random.fold_in(key, 11)
    key_level = jax.random.fold_in(key, 12)
    levels = jax.random.uniform(key_level, (HID,), jnp.float32, 0.0, 0.8)
    levels = levels + 0.48 * jnp.arange(HID, dtype=jnp.float32) / HID
    scales = 0.5 * 10.0 ** levels
    base = jnp.clip(jax.random.normal(key_base, (ROWS, HID), jnp.float32), -4.0, 4.0)
    return (base * scales[None, :]).astype(jnp.bfloat16)


def draw_delta(key, part):
    key_base = jax.random.fold_in(key, 21)
    key_rows = jax.random.fold_in(key, 22)
    key_cols = jax.random.fold_in(key, 23)
    owners = shuffled_clients(key).astype(jnp.float32) / CLIENTS
    col_levels = jax.random.uniform(key_cols, (EMIT,), jnp.float32, 0.0, 0.5)
    row_levels = jnp.repeat(owners, SPANS, total_repeat_length=ROWS)
    row_levels = row_levels + jax.random.uniform(key_rows, (ROWS,), jnp.float32, 0.0, 0.3)
    base = jnp.clip(jax.random.normal(key_base, (ROWS, EMIT), jnp.float32), -4.0, 4.0)
    values = base * (10.0 ** row_levels)[:, None] * (10.0 ** col_levels)[None, :]
    return values.astype(jnp.float32)


def shard_levels(stream_key, dims, shards, low, high):
    level, own = 1.0, jax.random.fold_in(stream_key, 6)
    for position, blocks in shards:
        heights = jnp.exp(jax.random.uniform(jax.random.fold_in(own, position), (blocks,), jnp.float32, low / len(shards), high / len(shards)))
        level = level * jnp.repeat(heights, dims[position] // blocks).reshape([-1 if axis == position else 1 for axis in range(len(dims))])
    return level


def gaussian(rng, shape, deviation, reach, cuts=(), kind=jnp.bfloat16):
    drawn = jax.random.normal(rng, shape, jnp.float32) * deviation
    if len(cuts) > 0:
        drawn = shard_levels(rng, shape, cuts, -0.22, 0.18) * drawn
    return jnp.clip(drawn, min=-reach, max=reach).astype(kind)


def setup_inputs(seed: int = 0) -> dict:
    key_of = jax.random.split(jax.random.key(seed), 5)
    pre = draw_pre(jax.random.fold_in(key_of[4], 71), 0)
    delta = draw_delta(jax.random.fold_in(key_of[4], 71), 0)
    head_weight = gaussian(key_of[2], (HID, EMIT), HID ** -0.5, 0.09375, ((1, 4),))
    client_ids = draw_client_ids(jax.random.fold_in(key_of[4], 71), 0)
    return {"pre": pre, "delta": delta, "head_weight": head_weight, "client_ids": client_ids}


def silu_slope(values):
    sigma = jax.nn.sigmoid(values)
    return sigma * (1.0 + values * (1.0 - sigma))

def clip_factor(total, number):
    return jnp.minimum(1.0, 1.0 / jnp.sqrt(total / number + 1e-06))

def reference(pre, delta, head_weight, client_ids):
    pre_wide = pre.astype(jnp.float32)
    hidden = jax.nn.silu(pre_wide).astype(jnp.bfloat16)
    delta_low = delta.astype(jnp.bfloat16)
    head_raw = jnp.dot(hidden.T, delta_low, preferred_element_type=jnp.float32)
    bias_raw = lax.optimization_barrier(jnp.sum(delta, axis=0))
    block = EMIT // N_HEAD
    hidden_grad = jnp.zeros((ROWS, HID), jnp.float32)
    for which in range(N_HEAD):
        partial_sum = jnp.dot(delta_low[:, which * block:(which + 1) * block], head_weight[:, which * block:(which + 1) * block].T, preferred_element_type=jnp.float32)
        rounded = lax.optimization_barrier(partial_sum.astype(jnp.bfloat16))
        hidden_grad = hidden_grad + rounded.astype(jnp.float32)
    pre_grad = hidden_grad * silu_slope(pre_wide)
    grouped = pre_grad.reshape(CLIENTS, SPANS, HID)
    client_part = lax.optimization_barrier(jnp.sum(grouped, axis=1))
    span_raw = lax.optimization_barrier(jnp.sum(grouped, axis=0))
    embed_raw = jnp.zeros((CLIENTS, HID), jnp.float32).at[client_ids.astype(jnp.int32)].add(client_part)
    head_factor = clip_factor(jnp.sum(head_raw * head_raw), HID * EMIT)
    embed_factor = clip_factor(jnp.sum(embed_raw * embed_raw), CLIENTS * HID)
    rest_total = jnp.sum(span_raw * span_raw) + jnp.sum(bias_raw * bias_raw)
    rest_factor = clip_factor(rest_total, SPANS * HID + EMIT)
    return (head_factor * head_raw, rest_factor * bias_raw, embed_factor * embed_raw, rest_factor * span_raw)
```

```python
import functools

import jax
import jax.numpy as jnp
from jax import lax
from jax.experimental import pallas as pl
from jax.experimental.pallas import tpu as pltpu
from jax.sharding import PartitionSpec as P

EPSILON = 1e-06
MESH = pl.DeviceIdType.MESH
F32 = jnp.float32
BF16 = jnp.bfloat16


def clip_factor(total, number):
    return jnp.minimum(1.0, 1.0 / jnp.sqrt(total / number + EPSILON))


def flip(index, mask, bits):
    out = 0
    for b in range(bits):
        i = (index // 2**b) % 2
        m = (mask // 2**b) % 2
        out = out + (i + m - 2 * i * m) * 2**b
    return out


def kernel(cfg, pre_ref, delta_ref, weight_ref, ids_ref, head_out, rest_out, embed_out, stat_out,
           pre_v, delta_v, low, weight_v, part, landed, small, small_in, mine, span_in, span_all,
           embed_all, ids_all, stat, stat_in, stat_head_in,
           pre_sem, delta_sem, weight_sem, tree_send, tree_recv, head_send, head_recv,
           span_send, span_recv, gather_send, gather_recv, embed_send, embed_recv,
           ids_send, ids_recv, stat_send, stat_recv):
    n, heads, q, piece, groups, spans, clients = cfg
    bits = n.bit_length() - 1
    block = q * piece
    half = n // 2 * q
    pieces = n * q
    me = lax.axis_index("client")
    my_head = lax.axis_index("head")
    emit = low.shape[1]

    barrier = pltpu.get_barrier_semaphore()
    for d in range(1, n):
        pl.semaphore_signal(barrier, inc=1, device_id={"client": lax.rem(me + d, n)}, device_id_type=MESH)
    for d in range(1, heads):
        pl.semaphore_signal(barrier, inc=1, device_id={"head": lax.rem(my_head + d, heads)}, device_id_type=MESH)

    def place(i):
        pos = i // q
        upper = pos // (n // 2)
        mask = n - 2 - 2 * (pos % (n // 2)) + 1 - upper
        row = flip(me, mask, bits) * block + (i % q) * piece
        return pl.multiple_of(row, piece)

    def pre_copy(i):
        return pltpu.make_async_copy(pre_ref.at[:, pl.ds(place(i), piece)], pre_v.at[i], pre_sem.at[i])

    delta_copy = pltpu.make_async_copy(delta_ref, delta_v, delta_sem)
    weight_copy = pltpu.make_async_copy(weight_ref, weight_v, weight_sem)
    delta_copy.start()
    ahead = 3
    for i in range(ahead):
        pre_copy(i).start()

    delta_copy.wait()
    step = 64
    def narrow(r, total):
        rows = pl.ds(pl.multiple_of(r * step, step), step)
        x = delta_v[rows, :]
        low[rows, :] = x.astype(BF16)
        return total + jnp.sum(x.reshape(step // 8, 8, emit), axis=0)
    bias = lax.fori_loop(0, low.shape[0] // step, narrow, jnp.zeros((8, emit), F32))
    bias = jnp.sum(bias, axis=0, keepdims=True)
    pad = groups * 16 - spans
    mine[pl.ds(spans, pad), :] = jnp.where(
        lax.broadcasted_iota(jnp.int32, (pad, emit), 0) == 0, jnp.broadcast_to(bias, (pad, emit)), 0.0
    ).astype(BF16)

    pl.semaphore_wait(barrier, n - 1 + heads - 1)

    def product(i):
        pre_copy(i).wait()
        p = pre_v[i].astype(F32)
        hidden = (p * jax.nn.sigmoid(p)).astype(BF16)
        value = lax.dot_general(hidden, low[...], (((0,), (0,)), ((), ())), preferred_element_type=F32)
        part[pl.ds(place(i), piece), :] = value.astype(BF16)

    def tree_copy(source_row, slot, stage):
        return pltpu.make_async_remote_copy(
            src_ref=part.at[pl.ds(source_row, piece), :], dst_ref=landed.at[slot],
            send_sem=tree_send.at[slot], recv_sem=tree_recv.at[slot],
            device_id={"client": flip(me, 2**stage, bits)}, device_id_type=MESH)

    def first_slot(i):
        return (n // 2 - 1 - i // q) * q + i % q

    def first(i, carry):
        pre_copy(i + ahead).start()
        product(i)
        tree_copy(place(i), first_slot(i), 0).start()
        return carry
    lax.fori_loop(0, half, first, 0)
    weight_copy.start()

    ids_copies = []
    for d in range(1, n):
        copy = pltpu.make_async_remote_copy(
            src_ref=ids_ref, dst_ref=ids_all.at[d],
            send_sem=ids_send.at[d], recv_sem=ids_recv.at[d],
            device_id={"client": lax.rem(me + d, n)}, device_id_type=MESH)
        copy.start()
        ids_copies.append(copy)

    def own(i, carry):
        @pl.when(i + ahead < pieces)
        def _():
            pre_copy(i + ahead).start()
        product(i)
        return carry
    lax.fori_loop(half, pieces, own, 0)
    weight_copy.wait()

    def slope_sums(i, carry):
        p = pre_v[i].astype(F32)
        row = place(i)
        value = lax.dot_general(
            low[...], weight_v[pl.ds(row, piece), :], (((1,), (1,)), ((), ())), preferred_element_type=F32)
        s = jax.nn.sigmoid(p)
        grad = value.astype(BF16).astype(F32) * (s * (1.0 + p * (1.0 - s)))
        grad = grad.reshape(clients, spans, piece)
        to = row // emit
        columns = pl.ds(pl.multiple_of(row % emit, piece), piece)
        small[to, pl.ds(0, spans), columns] = jnp.sum(grad, axis=0).astype(BF16)
        small[to, pl.ds(spans, clients), columns] = jnp.sum(grad, axis=1).astype(BF16)
        return carry

    bases = [0]
    for s in range(bits):
        bases.append(bases[-1] + (n >> (s + 1)) * q)
    later = []

    def combine(mask, sub):
        row = pl.multiple_of(flip(me, mask, bits) * block + sub * piece, piece)
        level = bits if mask == 0 else (mask & -mask).bit_length() - 1
        for s in range(level):
            slot = bases[s] + (mask >> (s + 1)) * q + sub
            tree_copy(row, slot, s).wait_recv()
        def chunk(r, carry):
            rows = min(64, piece)
            at = pl.multiple_of(r * rows, rows)
            total = part[pl.ds(pl.multiple_of(row + at, rows), rows), :].astype(F32)
            for s in range(level):
                slot = bases[s] + (mask >> (s + 1)) * q + sub
                total = total + landed[slot, pl.ds(at, rows), :].astype(F32)
            if mask == 0:
                head_out[pl.ds(pl.multiple_of(sub * piece + at, rows), rows), :] = total
                return carry + jnp.sum((total * total).reshape(rows // 8, 8, emit), axis=0)
            part[pl.ds(pl.multiple_of(row + at, rows), rows), :] = total.astype(BF16)
            return carry
        rows = min(64, piece)
        start = jnp.zeros((8, emit), F32)
        total = lax.fori_loop(0, piece // rows, chunk, start if mask == 0 else 0)
        if mask == 0:
            return total
        slot = bases[level] + (mask >> (level + 1)) * q + sub
        copy = tree_copy(row, slot, level)
        copy.start()
        later.append(copy)

    order = [(mask, sub) for mask in range(n - 2, -1, -2) for sub in range(q)]
    before = order[: 3 * len(order) // 8]
    middle = order[len(before): 3 * len(order) // 4]
    last = order[len(before) + len(middle):]
    for item in before:
        combine(*item)
    at = 0
    for k, item in enumerate(middle):
        upto = pieces * (k + 1) // len(middle)
        lax.fori_loop(at, upto, slope_sums, 0)
        at = upto
        if k == len(middle) - 1:
            head_copies = []
            for d in range(1, heads):
                target = lax.rem(my_head + d, heads)
                copy = pltpu.make_async_remote_copy(
                    src_ref=small.at[target], dst_ref=small_in.at[d - 1],
                    send_sem=head_send.at[d - 1], recv_sem=head_recv.at[d - 1],
                    device_id={"head": target}, device_id_type=MESH)
                copy.start()
                head_copies.append(copy)
        combine(*item)

    for copy in head_copies:
        copy.wait_recv()
    total = small[my_head].astype(F32)
    for d in range(heads - 1):
        total = total + small_in[d].astype(F32)
    mine[pl.ds(0, spans), :] = total[:spans].astype(BF16)
    embed_all[0] = total[spans:].astype(BF16)

    def span_copy(d):
        target = lax.rem(me + d, n)
        return target, pltpu.make_async_remote_copy(
            src_ref=mine.at[pl.ds(pl.multiple_of(lax.rem(target, groups) * 16, 16), 16), :],
            dst_ref=span_in.at[d], send_sem=span_send.at[d], recv_sem=span_recv.at[d],
            device_id={"client": target}, device_id_type=MESH)

    for d in range(1, n):
        target, copy = span_copy(d)
        @pl.when(target < groups)
        def _():
            copy.start()
    embed_copies = []
    for d in range(1, n):
        copy = pltpu.make_async_remote_copy(
            src_ref=embed_all.at[0], dst_ref=embed_all.at[d],
            send_sem=embed_send.at[d], recv_sem=embed_recv.at[d],
            device_id={"client": lax.rem(me + d, n)}, device_id_type=MESH)
        copy.start()
        embed_copies.append(copy)

    head_square = jnp.zeros((8, emit), F32)
    for item in last[: len(last) // 2]:
        value = combine(*item)
        head_square = head_square if value is None else head_square + value

    def gather_copy(d):
        slot = lax.rem(me, groups)
        return pltpu.make_async_remote_copy(
            src_ref=span_all.at[slot], dst_ref=span_all.at[slot],
            send_sem=gather_send.at[d], recv_sem=gather_recv.at[slot],
            device_id={"client": lax.rem(me + d, n)}, device_id_type=MESH)

    @pl.when(me < groups)
    def _():
        for d in range(1, n):
            span_copy(d)[1].wait_recv()
        total = mine[pl.ds(pl.multiple_of(lax.rem(me, groups) * 16, 16), 16), :].astype(F32)
        for d in range(1, n):
            total = total + span_in[d].astype(F32)
        span_all[lax.rem(me, groups)] = total.astype(BF16)
        for d in range(1, n):
            gather_copy(d).start()

    for copy in embed_copies + ids_copies:
        copy.wait_recv()
    wanted = lax.broadcasted_iota(jnp.int32, (clients, 128), 1) + me * clients
    embed_raw = jnp.zeros((clients, emit), F32)
    for d in range(n):
        ids = ids_ref[...] if d == 0 else ids_all[d]
        chosen = (ids == wanted).astype(F32).astype(BF16)
        picked = lax.dot_general(chosen, embed_all[d], (((0,), (0,)), ((), ())), preferred_element_type=F32)
        embed_raw = embed_raw + picked[:clients]
    embed_out[...] = embed_raw
    embed_square = jnp.sum(embed_raw * embed_raw)

    for g in range(groups):
        @pl.when(me != g)
        def _():
            pltpu.make_async_remote_copy(
                src_ref=span_all.at[g], dst_ref=span_all.at[g],
                send_sem=gather_send.at[0], recv_sem=gather_recv.at[g],
                device_id={"client": lax.rem(me + 1, n)}, device_id_type=MESH).wait_recv()
    rest_square = jnp.zeros((), F32)
    for g in range(groups):
        value = span_all[g].astype(F32)
        rest_out[pl.ds(16 * g, 16), :] = value
        rest_square = rest_square + jnp.sum(value * value)

    for item in last[len(last) // 2:]:
        value = combine(*item)
        head_square = head_square if value is None else head_square + value
    head_total = jnp.sum(head_square)

    line = lax.broadcasted_iota(jnp.int32, (8, 128), 0)
    stat[0] = jnp.where(line == 0, head_total, jnp.where(line == 1, embed_square, rest_square / n))
    copies = []
    for d in range(1, n):
        copy = pltpu.make_async_remote_copy(
            src_ref=stat.at[0], dst_ref=stat_in.at[d - 1], send_sem=stat_send.at[d - 1],
            recv_sem=stat_recv.at[d - 1], device_id={"client": lax.rem(me + d, n)}, device_id_type=MESH)
        copy.start()
        copies.append(copy)
    total = stat[0]
    for d, copy in enumerate(copies):
        copy.wait_recv()
        total = total + stat_in[d]
    stat[1] = total
    more = []
    for d in range(1, heads):
        slot = n - 2 + d
        copy = pltpu.make_async_remote_copy(
            src_ref=stat.at[1], dst_ref=stat_head_in.at[d - 1], send_sem=stat_send.at[slot],
            recv_sem=stat_recv.at[slot], device_id={"head": lax.rem(my_head + d, heads)}, device_id_type=MESH)
        copy.start()
        more.append(copy)
    for d, copy in enumerate(more):
        copy.wait_recv()
        total = total + stat_head_in[d]
    stat_out[...] = total

    def sent(i, carry):
        tree_copy(place(i), first_slot(i), 0).wait_send()
        return carry
    lax.fori_loop(0, half, sent, 0)
    for copy in later + head_copies + embed_copies + ids_copies + copies + more:
        copy.wait_send()
    for d in range(1, n):
        target, copy = span_copy(d)
        @pl.when(target < groups)
        def _():
            copy.wait_send()
    @pl.when(me < groups)
    def _():
        for d in range(1, n):
            gather_copy(d).wait_send()


def per_device(n, heads, pre, delta, head_weight, client_ids):
    rows, hidden_width = pre.shape
    emit = delta.shape[1]
    clients = client_ids.shape[0]
    spans = rows // clients
    block = hidden_width // n
    piece = min(256, block)
    q = block // piece
    groups = (spans + 16) // 16
    cfg = (n, heads, q, piece, groups, spans, clients)
    ids = jnp.broadcast_to(client_ids[:, None], (clients, 128))
    hbm = pl.BlockSpec(memory_space=pl.ANY)
    vmem = pl.BlockSpec(memory_space=pltpu.VMEM)
    dma = pltpu.SemaphoreType.DMA
    slots = (n - 1) * q
    head_raw, rest_raw, embed_raw, stats = pl.pallas_call(
        functools.partial(kernel, cfg),
        out_shape=(
            jax.ShapeDtypeStruct((block, emit), F32),
            jax.ShapeDtypeStruct((groups * 16, emit), F32),
            jax.ShapeDtypeStruct((clients, emit), F32),
            jax.ShapeDtypeStruct((8, 128), F32),
        ),
        in_specs=[hbm, hbm, hbm, vmem],
        out_specs=(vmem, vmem, vmem, vmem),
        scratch_shapes=[
            pltpu.VMEM((n * q, rows, piece), BF16),
            pltpu.VMEM((rows, emit), F32),
            pltpu.VMEM((rows, emit), BF16),
            pltpu.VMEM((hidden_width, emit), BF16),
            pltpu.VMEM((hidden_width, emit), BF16),
            pltpu.VMEM((slots, piece, emit), BF16),
            pltpu.VMEM((heads, spans + clients, emit), BF16),
            pltpu.VMEM((heads - 1, spans + clients, emit), BF16),
            pltpu.VMEM((groups * 16, emit), BF16),
            pltpu.VMEM((n, 16, emit), BF16),
            pltpu.VMEM((groups, 16, emit), BF16),
            pltpu.VMEM((n, clients, emit), BF16),
            pltpu.VMEM((n, clients, 128), jnp.int32),
            pltpu.VMEM((2, 8, 128), F32),
            pltpu.VMEM((n - 1, 8, 128), F32),
            pltpu.VMEM((heads - 1, 8, 128), F32),
            dma((n * q,)), dma, dma, dma((slots,)), dma((slots,)),
            dma((heads - 1,)), dma((heads - 1,)),
            dma((n,)), dma((n,)), dma((n,)), dma((groups,)), dma((n,)), dma((n,)),
            dma((n,)), dma((n,)), dma((n + heads - 2,)), dma((n + heads - 2,)),
        ],
        compiler_params=pltpu.CompilerParams(
            collective_id=0, has_side_effects=True, vmem_limit_bytes=60 * 2**20
        ),
        name="clipped_grads",
    )(pre, delta, head_weight, ids)
    head_factor = clip_factor(stats[0, 0], hidden_width * emit * heads)
    embed_factor = clip_factor(stats[1, 0], clients * n * hidden_width)
    rest_factor = clip_factor(stats[2, 0], spans * hidden_width + emit * heads)
    return (
        head_factor * head_raw,
        rest_factor * rest_raw[spans],
        embed_factor * embed_raw,
        rest_factor * rest_raw[:spans],
    )


def solution(mesh):
    placed = (P("client", None), P("client", "head"), P(None, "head"), P("client"))
    return jax.shard_map(
        functools.partial(per_device, mesh.shape["client"], mesh.shape["head"]),
        mesh=mesh,
        in_specs=placed,
        out_specs=(P("client", "head"), P("head"), P("client", "head"), P(None, "head")),
        check_vma=False,
    )
```
